32 devices in a mesh: pair: 8 (over z, core), orb: 4 (over y, x).
Axes of the slice: x: 2, y: 2, z: 4, core: 2. Of those that a mesh axis runs over, the one named last changes fastest.
Arguments:
- amplitudes: float32 [128, 128, 128], P(('pair', 'orb')), may hold values from -3 to 3
- couple: int32 [128, 16], P(('pair', 'orb')), may hold values from 0 to 127, as said below
- occ_first: int32 [128], P('pair'), may hold values from 0 to 31, as said below
- occ_second: int32 [128], P('pair'), may hold values from 0 to 31, as said below
- couple_intersection: bfloat16 [128, 16, 128, 128], P(('pair', 'orb')), may hold values from -0.375 to 0.375
- pno_maps: bfloat16 [128, 2, 128, 128], P('pair'), may hold values from -0.5 to 0.5
- orbital_blocks: bfloat16 [32, 512, 128], P('pair', 'orb'), may hold values from -2 to 2
- pno_energy: float32 [128, 128], P(('pair', 'orb')), may hold values from 0.5 to 2.5
- occ_energy: float32 [32], replicated, may hold values from -1.5 to -0.3
Outputs:
- new_amplitudes: float32 [128, 128, 128], P(('pair', 'orb'))
- dressed: float32 [32, 512, 128], P('pair', 'orb')
The draws below stay inside these ranges and needn't reach their ends.
Inputs may be any that keep to these rules, and one draw needn't show every extreme that they name: `couple`: every listed partner of a pair lies in the same pair group as the pair (pairs g * 16 to (g + 1) * 16 - 1 form group g). `occ_first`: the pairs of group g have first orbitals in g * 4 to (g + 1) * 4 - 1. `occ_second`: the pairs of group g have second orbitals among the orbitals of groups g - 1 to g + 1, counted modulo 8 (group h holds orbitals h * 4 to (h + 1) * 4 - 1).
All inputs are finite; a program needn't handle non-finite values.
Results may differ from the reference program's by a relative error of at most 0.014.
Values may be sent and summed in bfloat16 or wider, within the bound.
A program may use at most 64 MiB of HBM per device.

```python
import math
import jax
import jax.numpy as jnp
from jax import lax

P_SIZE = 128
Q = 512
ORB_DEV = 4
KC = 16
REACH = 1
ITERS = 2
PAIR_GRP = 16
NPAIR = 128
NORB = 32
N_ORB = 4


def draw_couple(key, part):
    group_ids = jnp.arange(NPAIR, dtype=jnp.int32) // PAIR_GRP
    picked = jax.random.randint(jax.random.fold_in(key, 1), (NPAIR, KC), 0, PAIR_GRP, dtype=jnp.int32)
    return group_ids[:, None] * PAIR_GRP + picked


def draw_occ_first(key, part):
    group_ids = jnp.arange(NPAIR, dtype=jnp.int32) // PAIR_GRP
    picked = jax.random.randint(jax.random.fold_in(key, 3), (NPAIR,), 0, ORB_DEV, dtype=jnp.int32)
    return group_ids * ORB_DEV + picked


def draw_occ_second(key, part):
    groups = NPAIR // PAIR_GRP
    key_step, key_local = jax.random.split(jax.random.fold_in(key, 7), 2)
    steps_drawn = jax.random.randint(key_step, (groups, PAIR_GRP), 0, 2 * REACH + 1, dtype=jnp.int32)
    column = jnp.arange(PAIR_GRP, dtype=jnp.int32)[None, :]
    steps_drawn = jnp.where(column < 2 * REACH + 1, column, steps_drawn)
    group_ids = jnp.arange(groups, dtype=jnp.int32)[:, None]
    owner_ids = (group_ids + steps_drawn - REACH + groups) % groups
    local_ids = jax.random.randint(key_local, (groups, PAIR_GRP), 0, ORB_DEV, dtype=jnp.int32)
    return (owner_ids * ORB_DEV + local_ids).reshape(NPAIR)


def block_levels(own_key, extent, cuts, least, top_value):
    def one(axis_at, parts):
        heights = jax.random.uniform(jax.random.fold_in(jax.random.fold_in(own_key, 6), axis_at), (parts,), jnp.float32, least / len(cuts), top_value / len(cuts))
        return jnp.repeat(jnp.exp(heights), extent[axis_at] // parts).reshape((-1,) + (1,) * (len(extent) - axis_at - 1))

    factor_of = one(*cuts[0])
    for cut in cuts[1:]:
        factor_of = factor_of * one(*cut)
    return factor_of


def noise(rng, shape, width, most, cuts=(), kind=jnp.bfloat16):
    array = jax.random.normal(rng, shape, jnp.float32) * width
    if len(cuts) > 0:
        array = block_levels(rng, shape, cuts, -0.22, 0.18) * array
    return jnp.clip(array, min=-most, max=most).astype(kind)


def setup_inputs(seed: int = 0) -> dict:
    seeds = jax.random.split(jax.random.key(seed), 10)
    amplitudes = noise(seeds[0], (NPAIR, P_SIZE, P_SIZE), 0.5, 3.0, ((0, 32),), jnp.float32)
    couple = draw_couple(jax.random.fold_in(seeds[9], 71), 0)
    occ_first = draw_occ_first(jax.random.fold_in(seeds[9], 71), 0)
    occ_second = draw_occ_second(jax.random.fold_in(seeds[9], 71), 0)
    couple_intersection = noise(seeds[4], (NPAIR, KC, P_SIZE, P_SIZE), (2 * P_SIZE) ** -0.5, 0.375, ((0, 32),))
    pno_maps = noise(seeds[5], (NPAIR, 2, P_SIZE, P_SIZE), P_SIZE ** -0.5, 0.5, ((0, 8),))
    orbital_blocks = noise(seeds[6], (NORB, Q, P_SIZE), 0.3, 2.0, ((0, 8), (1, 4)))
    pno_energy = jnp.clip(jnp.exp(math.log(2.5) - 1.609438 * jax.random.uniform(seeds[7], (NPAIR, P_SIZE), jnp.float32) ** block_levels(seeds[7], (NPAIR, P_SIZE), ((0, 32),), -0.2, 0.2)), 0.5, 2.5)
    occ_energy = jnp.clip(jax.random.uniform(seeds[8], (NORB,), jnp.float32, -1.5, -0.3), -1.5, -0.3)
    return dict(amplitudes=amplitudes, couple=couple, occ_first=occ_first, occ_second=occ_second, couple_intersection=couple_intersection, pno_maps=pno_maps, orbital_blocks=orbital_blocks, pno_energy=pno_energy, occ_energy=occ_energy)


dress_scale = 0.015


def as_float(values):
    return values.astype(jnp.float32)


def reference(amplitudes, couple, occ_first, occ_second, couple_intersection, pno_maps, orbital_blocks, pno_energy, occ_energy):
    slice_rows = Q // N_ORB
    block_total = NPAIR // PAIR_GRP
    denominator = pno_energy[:, :, None] + pno_energy[:, None, :]
    denominator = denominator - occ_energy[occ_first][:, None, None] - occ_energy[occ_second][:, None, None]
    bare_blocks = as_float(orbital_blocks)
    dressed = bare_blocks
    amps_now = amplitudes
    highest = lax.Precision.HIGHEST
    for iteration in range(ITERS):
        amp_half = amps_now.astype(jnp.bfloat16)
        block_half = dressed.astype(jnp.bfloat16)

        def one_block(fitted, block_index):
            first_row = (block_index * PAIR_GRP).astype(jnp.int32)
            first_ids = lax.dynamic_slice_in_dim(occ_first, first_row, PAIR_GRP)
            second_ids = lax.dynamic_slice_in_dim(occ_second, first_row, PAIR_GRP)
            pair_maps = as_float(lax.dynamic_slice_in_dim(pno_maps, first_row, PAIR_GRP))
            first_proj = jnp.einsum("pqa,pab->pqb", as_float(block_half[first_ids]), pair_maps[:, 0], precision=highest).astype(jnp.bfloat16)
            second_proj = jnp.einsum("pqa,pab->pqb", as_float(block_half[second_ids]), pair_maps[:, 1], precision=highest).astype(jnp.bfloat16)
            left_parts = as_float(first_proj).reshape(PAIR_GRP, N_ORB, slice_rows, P_SIZE)
            right_parts = as_float(second_proj).reshape(PAIR_GRP, N_ORB, slice_rows, P_SIZE)
            partial_value = jnp.einsum("psqa,psqb->psab", left_parts, right_parts, precision=highest)
            integrals = jnp.sum(as_float(partial_value.astype(jnp.bfloat16)), axis=1)
            partner_ids = lax.dynamic_slice_in_dim(couple, first_row, PAIR_GRP)
            partners = as_float(amp_half[partner_ids])
            intersection = as_float(lax.dynamic_slice_in_dim(couple_intersection, first_row, PAIR_GRP))
            half_products = jnp.einsum("pkab,pkbc->pkac", intersection, partners, precision=highest).astype(jnp.bfloat16)
            coupled = jnp.einsum("pkac,pkdc->pad", as_float(half_products), intersection, precision=highest)
            own_amps = as_float(lax.dynamic_slice_in_dim(amp_half, first_row, PAIR_GRP))
            fitted_half = jnp.einsum("pqa,pab->pqb", as_float(second_proj), own_amps, precision=highest).astype(jnp.bfloat16)
            returned = jnp.einsum("pqb,pcb->pqc", as_float(fitted_half), pair_maps[:, 0], precision=highest)
            fitted = fitted.at[first_ids].add(returned)
            return fitted, integrals + coupled

        start_fitted = jnp.zeros((NORB, Q, P_SIZE), jnp.float32)
        fitted, driving = lax.scan(one_block, start_fitted, jnp.arange(block_total, dtype=jnp.int32))
        driving = driving.reshape(NPAIR, P_SIZE, P_SIZE)
        dressed = bare_blocks + dress_scale * fitted
        amps_now = -driving / denominator
    return amps_now, dressed
```

```python
import functools

import jax
import jax.numpy as jnp
from jax import lax
from jax.experimental import pallas as pl
from jax.experimental.pallas import tpu as pltpu
from jax.sharding import PartitionSpec as P

REACH = 1
ITERS = 2
SIDES = 2 * REACH + 1

dress_scale = 0.015

NN = (((1,), (0,)), ((), ()))
NT = (((1,), (1,)), ((), ()))


def dot(left, right, dims=NN):
    return lax.dot_general(left, right, dims, preferred_element_type=jnp.float32)


def kernel(
    ranks,
    groups,
    couple,
    occ_first,
    occ_second,
    occ_energy,
    amplitudes,
    pno_energy,
    inter_hbm,
    maps_hbm,
    orb_hbm,
    out_amps,
    out_dressed,
    inter,
    maps,
    first_t,
    amps_0,
    amps_1,
    window_0,
    window_1,
    second_z,
    parts_out,
    parts_in,
    half,
    fitted,
    amp_send,
    amp_recv,
    win_send,
    win_recv,
    part_send,
    part_recv,
    inter_sem,
    maps_sem,
    orb_sem,
):
    amps = (amps_0, amps_1)
    window = (window_0, window_1)
    own_pairs = amplitudes.shape[0]
    orbs = orb_hbm.shape[0]
    partners = couple.shape[1]
    size = amplitudes.shape[2]
    me = lax.axis_index("orb")
    group = lax.axis_index("pair")
    own = me * own_pairs
    own_rows = pl.ds(own, own_pairs)
    middle = pl.ds(REACH * orbs, orbs)
    bf16 = jnp.bfloat16

    orb_copy = pltpu.make_async_copy(orb_hbm, window[0].at[middle], orb_sem)
    orb_copy.start()
    maps_copies = []
    for part in range(2):
        chunk = pl.ds(part * (maps.shape[0] // 2), maps.shape[0] // 2)
        maps_copies.append(
            pltpu.make_async_copy(maps_hbm.at[chunk], maps.at[chunk], maps_sem.at[part])
        )
        maps_copies[-1].start()
    inter_copies = []
    for i in range(own_pairs):
        inter_copies.append(pltpu.make_async_copy(inter_hbm.at[i], inter.at[i], inter_sem.at[i]))
        inter_copies[-1].start()

    for i in range(own_pairs):
        amps[0][own + i] = amplitudes[i].astype(bf16)

    barrier = pltpu.get_barrier_semaphore()
    for step in range(1, ranks):
        pl.semaphore_signal(
            barrier,
            inc=1,
            device_id={"orb": (me + step) % ranks},
            device_id_type=pl.DeviceIdType.MESH,
        )
    for step in range(1, REACH + 1):
        for shift in (step, groups - step):
            pl.semaphore_signal(
                barrier,
                inc=1,
                device_id={"pair": (group + shift) % groups},
                device_id_type=pl.DeviceIdType.MESH,
            )
    pl.semaphore_wait(barrier, ranks - 1 + 2 * REACH)

    def win_copy(turn, place):
        return pltpu.make_async_remote_copy(
            src_ref=window[turn].at[middle],
            dst_ref=window[turn].at[pl.ds(place * orbs, orbs)],
            send_sem=win_send.at[turn, place],
            recv_sem=win_recv.at[turn, place],
            device_id={"pair": (group + REACH - place + groups) % groups},
            device_id_type=pl.DeviceIdType.MESH,
        )

    def amp_copy(turn, step, i):
        return pltpu.make_async_remote_copy(
            src_ref=amps[turn].at[own + i],
            dst_ref=amps[turn].at[own + i],
            send_sem=amp_send.at[turn, step, i],
            recv_sem=amp_recv.at[turn, step, i],
            device_id={"orb": (me + step) % ranks},
            device_id_type=pl.DeviceIdType.MESH,
        )

    def amp_wait(turn, step):
        for i in range(own_pairs):
            amp_copy(turn, step, i).wait_recv()

    def part_copy(turn, step):
        return pltpu.make_async_remote_copy(
            src_ref=parts_out.at[turn, step],
            dst_ref=parts_in.at[turn, step],
            send_sem=part_send.at[turn, step],
            recv_sem=part_recv.at[turn, step],
            device_id={"orb": (me + step) % ranks},
            device_id_type=pl.DeviceIdType.MESH,
        )

    places = [place for place in range(SIDES) if place != REACH]

    orb_copy.wait()
    for place in places:
        win_copy(0, place).start()
    for step in range(1, ranks):
        for i in range(own_pairs):
            amp_copy(0, step, i).start()

    for copy in maps_copies:
        copy.wait()

    @pl.loop(0, ranks)
    def _(block):
        for i in range(own_pairs):
            first_t[block * own_pairs + i] = maps[block * own_pairs + i, 0].T

    for turn in range(ITERS):
        for place in places:
            win_copy(turn, place).wait_recv()

        @pl.loop(1, ranks + 1)
        def _(ahead):
            step = ahead % ranks
            base = ((me + step) % ranks) * own_pairs
            lefts, rights = [], []
            for i in range(own_pairs):
                pair = base + i
                first = REACH * orbs + occ_first[pair] % orbs
                second = occ_second[pair]
                distance = (second // orbs - group + REACH + groups) % groups
                place = jnp.minimum(distance, SIDES - 1)
                lefts.append(dot(first_t[pair], window[turn][first], NT).astype(bf16))
                rights.append(
                    dot(window[turn][place * orbs + second % orbs], maps[pair, 1]).astype(bf16)
                )
            for i in range(own_pairs):
                second_z[base + i] = rights[i]
                parts_out[turn, step, i] = dot(lefts[i], rights[i]).astype(bf16)

            @pl.when(ahead < ranks)
            def _():
                part_copy(turn, step).start()

        for o in range(orbs):
            fitted[o] = jnp.zeros_like(fitted[o])

        @pl.loop(0, ranks)
        def _(step):
            @pl.when(step > 0)
            def _():
                amp_wait(turn, step)

            base = ((me + ranks - step) % ranks) * own_pairs
            halves = [
                dot(second_z[base + i], amps[turn][base + i]).astype(bf16)
                for i in range(own_pairs)
            ]
            returned = [dot(halves[i], first_t[base + i]) for i in range(own_pairs)]
            for o in range(orbs):
                total = fitted[o]
                for i in range(own_pairs):
                    weight = (occ_first[base + i] % orbs == o).astype(jnp.float32)
                    total += weight * returned[i]
                fitted[o] = total

        for o in range(orbs):
            value = window[0][REACH * orbs + o].astype(jnp.float32) + dress_scale * fitted[o]
            if turn + 1 < ITERS:
                window[turn + 1][REACH * orbs + o] = value.astype(bf16)
            else:
                out_dressed[o] = value
        if turn + 1 < ITERS:
            for place in places:
                win_copy(turn + 1, place).start()

        if turn == 0:
            for copy in inter_copies:
                copy.wait()

        @pl.loop(0, own_pairs)
        def _(i):
            for k in range(partners):
                partner = couple[i, k] % (ranks * own_pairs)
                half[i, :, k * size : (k + 1) * size] = dot(
                    inter[i, k], amps[turn][partner]
                ).astype(bf16)
            coupled = None
            for k in range(0, partners, 2):
                right = jnp.concatenate([inter[i, k], inter[i, k + 1]], axis=1)
                term = dot(half[i, :, k * size : (k + 2) * size], right, NT)
                coupled = term if coupled is None else coupled + term

            @pl.when(i == 0)
            def _():
                for step in range(1, ranks):
                    part_copy(turn, step).wait_recv()

            total = parts_out[turn, 0, i].astype(jnp.float32)
            for step in range(1, ranks):
                total += parts_in[turn, step, i].astype(jnp.float32)
            rows = jnp.broadcast_to(pno_energy[pl.ds(i, 1), :], (size, size))
            denominator = rows + rows.T
            denominator -= occ_energy[occ_first[own + i]]
            denominator -= occ_energy[occ_second[own + i]]
            value = -(total + coupled) / denominator
            if turn + 1 < ITERS:
                amps[turn + 1][own + i] = value.astype(bf16)
                for step in range(1, ranks):
                    amp_copy(turn + 1, step, i).start()
            else:
                out_amps[i] = value

    for turn in range(ITERS):
        for place in places:
            win_copy(turn, place).wait_send()
        for step in range(1, ranks):
            part_copy(turn, step).wait_send()
            for i in range(own_pairs):
                amp_copy(turn, step, i).wait_send()


def on_device(
    ranks,
    groups,
    amplitudes,
    couple,
    occ_first,
    occ_second,
    couple_intersection,
    pno_maps,
    orbital_blocks,
    pno_energy,
    occ_energy,
):
    own_pairs, size, _ = amplitudes.shape
    group_pairs = occ_first.shape[0]
    orbs, rows, virtuals = orbital_blocks.shape
    partners = couple.shape[1]
    bf16 = jnp.bfloat16
    smem = pl.BlockSpec(memory_space=pltpu.SMEM)
    vmem = pl.BlockSpec(memory_space=pltpu.VMEM)
    hbm = pl.BlockSpec(memory_space=pl.ANY)
    dma = pltpu.SemaphoreType.DMA
    return pl.pallas_call(
        functools.partial(kernel, ranks, groups),
        out_shape=(
            jax.ShapeDtypeStruct(amplitudes.shape, jnp.float32),
            jax.ShapeDtypeStruct(orbital_blocks.shape, jnp.float32),
        ),
        in_specs=[smem] * 4 + [vmem] * 2 + [hbm] * 3,
        out_specs=(vmem, vmem),
        scratch_shapes=[
            pltpu.VMEM(couple_intersection.shape, bf16),
            pltpu.VMEM(pno_maps.shape, bf16),
            pltpu.VMEM((group_pairs, size, virtuals), bf16),
            pltpu.VMEM((group_pairs, size, size), bf16),
            pltpu.VMEM((group_pairs, size, size), bf16),
            pltpu.VMEM((SIDES * orbs, rows, virtuals), bf16),
            pltpu.VMEM((SIDES * orbs, rows, virtuals), bf16),
            pltpu.VMEM((group_pairs, rows, size), bf16),
            pltpu.VMEM((ITERS, ranks, own_pairs, size, size), bf16),
            pltpu.VMEM((ITERS, ranks, own_pairs, size, size), bf16),
            pltpu.VMEM((own_pairs, size, partners * size), bf16),
            pltpu.VMEM((orbs, rows, virtuals), jnp.float32),
            dma((ITERS, ranks, own_pairs)),
            dma((ITERS, ranks, own_pairs)),
            dma((ITERS, SIDES)),
            dma((ITERS, SIDES)),
            dma((ITERS, ranks)),
            dma((ITERS, ranks)),
            dma((own_pairs,)),
            dma((2,)),
            dma,
        ],
        compiler_params=pltpu.CompilerParams(
            collective_id=0, has_side_effects=True, vmem_limit_bytes=48 * 2**20
        ),
    )(
        couple,
        occ_first,
        occ_second,
        occ_energy,
        amplitudes,
        pno_energy,
        couple_intersection,
        pno_maps,
        orbital_blocks,
    )


def solution(mesh):
    return jax.shard_map(
        functools.partial(on_device, mesh.shape["orb"], mesh.shape["pair"]),
        mesh=mesh,
        in_specs=(
            P(("pair", "orb"), None, None),
            P(("pair", "orb"), None),
            P("pair"),
            P("pair"),
            P(("pair", "orb"), None, None, None),
            P("pair", None, None, None),
            P("pair", "orb", None),
            P(("pair", "orb"), None),
            P(),
        ),
        out_specs=(P(("pair", "orb"), None, None), P("pair", "orb", None)),
        check_vma=False,
    )
```

```python
import functools

import jax
import jax.numpy as jnp
from jax import lax
from jax.experimental import pallas as pl
from jax.experimental.pallas import tpu as pltpu
from jax.sharding import PartitionSpec as P

REACH = 1
ITERS = 2
SIDES = 2 * REACH + 1

dress_scale = 0.015

NN = (((1,), (0,)), ((), ()))
NT = (((1,), (1,)), ((), ()))


def dot(left, right, dims=NN):
    return lax.dot_general(left, right, dims, preferred_element_type=jnp.float32)


def kernel(
    ranks,
    groups,
    couple,
    occ_first,
    occ_second,
    occ_energy,
    amplitudes,
    pno_energy,
    inter_hbm,
    maps_hbm,
    orb_hbm,
    out_amps,
    out_dressed,
    inter,
    maps,
    first_t,
    amps_0,
    amps_1,
    window_0,
    window_1,
    second_z,
    parts_out,
    parts_in,
    half,
    fitted,
    amp_send,
    amp_recv,
    win_send,
    win_recv,
    part_send,
    part_recv,
    inter_sem,
    maps_sem,
    orb_sem,
):
    amps = (amps_0, amps_1)
    window = (window_0, window_1)
    own_pairs = amplitudes.shape[0]
    orbs = orb_hbm.shape[0]
    partners = couple.shape[1]
    size = amplitudes.shape[2]
    me = lax.axis_index("orb")
    group = lax.axis_index("pair")
    own = me * own_pairs
    own_rows = pl.ds(own, own_pairs)
    middle = pl.ds(REACH * orbs, orbs)
    bf16 = jnp.bfloat16

    orb_copy = pltpu.make_async_copy(orb_hbm, window[0].at[middle], orb_sem)
    orb_copy.start()
    maps_copies = []
    for part in range(2):
        chunk = pl.ds(part * (maps.shape[0] // 2), maps.shape[0] // 2)
        maps_copies.append(
            pltpu.make_async_copy(maps_hbm.at[chunk], maps.at[chunk], maps_sem.at[part])
        )
        maps_copies[-1].start()
    inter_copies = []
    for i in range(own_pairs):
        inter_copies.append(pltpu.make_async_copy(inter_hbm.at[i], inter.at[i], inter_sem.at[i]))
        inter_copies[-1].start()

    for i in range(own_pairs):
        amps[0][own + i] = amplitudes[i].astype(bf16)

    barrier = pltpu.get_barrier_semaphore()
    for step in range(1, ranks):
        pl.semaphore_signal(
            barrier,
            inc=1,
            device_id={"orb": (me + step) % ranks},
            device_id_type=pl.DeviceIdType.MESH,
        )
    for step in range(1, REACH + 1):
        for shift in (step, groups - step):
            pl.semaphore_signal(
                barrier,
                inc=1,
                device_id={"pair": (group + shift) % groups},
                device_id_type=pl.DeviceIdType.MESH,
            )
    pl.semaphore_wait(barrier, ranks - 1 + 2 * REACH)

    def win_copy(turn, place):
        return pltpu.make_async_remote_copy(
            src_ref=window[turn].at[middle],
            dst_ref=window[turn].at[pl.ds(place * orbs, orbs)],
            send_sem=win_send.at[turn, place],
            recv_sem=win_recv.at[turn, place],
            device_id={"pair": (group + REACH - place + groups) % groups},
            device_id_type=pl.DeviceIdType.MESH,
        )

    def amp_copy(turn, step, i):
        return pltpu.make_async_remote_copy(
            src_ref=amps[turn].at[own + i],
            dst_ref=amps[turn].at[own + i],
            send_sem=amp_send.at[turn, step, i],
            recv_sem=amp_recv.at[turn, step, i],
            device_id={"orb": (me + step) % ranks},
            device_id_type=pl.DeviceIdType.MESH,
        )

    def amp_wait(turn, step):
        for i in range(own_pairs):
            amp_copy(turn, step, i).wait_recv()

    def part_copy(turn, step):
        return pltpu.make_async_remote_copy(
            src_ref=parts_out.at[turn, step],
            dst_ref=parts_in.at[turn, step],
            send_sem=part_send.at[turn, step],
            recv_sem=part_recv.at[turn, step],
            device_id={"orb": (me + step) % ranks},
            device_id_type=pl.DeviceIdType.MESH,
        )

    places = [place for place in range(SIDES) if place != REACH]

    orb_copy.wait()
    for place in places:
        win_copy(0, place).start()
    for step in range(1, ranks):
        for i in range(own_pairs):
            amp_copy(0, step, i).start()

    for copy in maps_copies:
        copy.wait()

    @pl.loop(0, ranks)
    def _(block):
        for i in range(own_pairs):
            first_t[block * own_pairs + i] = maps[block * own_pairs + i, 0].T

    for turn in range(ITERS):
        for place in places:
            win_copy(turn, place).wait_recv()

        @pl.loop(1, ranks + 1)
        def _(ahead):
            step = ahead % ranks
            base = ((me + step) % ranks) * own_pairs
            lefts, rights = [], []
            for i in range(own_pairs):
                pair = base + i
                first = REACH * orbs + occ_first[pair] % orbs
                second = occ_second[pair]
                distance = (second // orbs - group + REACH + groups) % groups
                place = jnp.minimum(distance, SIDES - 1)
                lefts.append(dot(first_t[pair], window[turn][first], NT).astype(bf16))
                rights.append(
                    dot(window[turn][place * orbs + second % orbs], maps[pair, 1]).astype(bf16)
                )
            for i in range(own_pairs):
                second_z[base + i] = rights[i]
                parts_out[turn, step, i] = dot(lefts[i], rights[i]).astype(bf16)

            @pl.when(ahead < ranks)
            def _():
                part_copy(turn, step).start()

        for o in range(orbs):
            fitted[o] = jnp.zeros_like(fitted[o])

        @pl.loop(0, ranks)
        def _(step):
            @pl.when(step > 0)
            def _():
                amp_wait(turn, step)

            base = ((me + ranks - step) % ranks) * own_pairs
            halves = [
                dot(second_z[base + i], amps[turn][base + i]).astype(bf16)
                for i in range(own_pairs)
            ]
            returned = [dot(halves[i], first_t[base + i]) for i in range(own_pairs)]
            for o in range(orbs):
                total = fitted[o]
                for i in range(own_pairs):
                    weight = (occ_first[base + i] % orbs == o).astype(jnp.float32)
                    total += weight * returned[i]
                fitted[o] = total

        for o in range(orbs):
            value = window[0][REACH * orbs + o].astype(jnp.float32) + dress_scale * fitted[o]
            if turn + 1 < ITERS:
                window[turn + 1][REACH * orbs + o] = value.astype(bf16)
            else:
                out_dressed[o] = value
        if turn + 1 < ITERS:
            for place in places:
                win_copy(turn + 1, place).start()

        if turn == 0:
            for copy in inter_copies:
                copy.wait()

        @pl.loop(0, own_pairs)
        def _(i):
            for k in range(partners):
                partner = couple[i, k] % (ranks * own_pairs)
                half[i, :, k * size : (k + 1) * size] = dot(
                    inter[i, k], amps[turn][partner]
                ).astype(bf16)
            coupled = None
            for k in range(0, partners, 2):
                right = jnp.concatenate([inter[i, k], inter[i, k + 1]], axis=1)
                term = dot(half[i, :, k * size : (k + 2) * size], right, NT)
                coupled = term if coupled is None else coupled + term

            @pl.when(i == 0)
            def _():
                for step in range(1, ranks):
                    part_copy(turn, step).wait_recv()

            total = parts_out[turn, 0, i].astype(jnp.float32)
            for step in range(1, ranks):
                total += parts_in[turn, step, i].astype(jnp.float32)
            rows = jnp.broadcast_to(pno_energy[pl.ds(i, 1), :], (size, size))
            denominator = rows + rows.T
            denominator -= occ_energy[occ_first[own + i]]
            denominator -= occ_energy[occ_second[own + i]]
            value = -(total + coupled) / denominator
            if turn + 1 < ITERS:
                amps[turn + 1][own + i] = value.astype(bf16)
                for step in range(1, ranks):
                    amp_copy(turn + 1, step, i).start()
            else:
                out_amps[i] = value

    for turn in range(ITERS):
        for place in places:
            win_copy(turn, place).wait_send()
        for step in range(1, ranks):
            part_copy(turn, step).wait_send()
            for i in range(own_pairs):
                amp_copy(turn, step, i).wait_send()


def on_device(
    ranks,
    groups,
    amplitudes,
    couple,
    occ_first,
    occ_second,
    couple_intersection,
    pno_maps,
    orbital_blocks,
    pno_energy,
    occ_energy,
):
    own_pairs, size, _ = amplitudes.shape
    group_pairs = occ_first.shape[0]
    orbs, rows, virtuals = orbital_blocks.shape
    partners = couple.shape[1]
    bf16 = jnp.bfloat16
    smem = pl.BlockSpec(memory_space=pltpu.SMEM)
    vmem = pl.BlockSpec(memory_space=pltpu.VMEM)
    hbm = pl.BlockSpec(memory_space=pltpu.HBM)
    dma = pltpu.SemaphoreType.DMA
    return pl.pallas_call(
        functools.partial(kernel, ranks, groups),
        out_shape=(
            jax.ShapeDtypeStruct(amplitudes.shape, jnp.float32),
            jax.ShapeDtypeStruct(orbital_blocks.shape, jnp.float32),
        ),
        in_specs=[smem] * 4 + [vmem] * 2 + [hbm] * 3,
        out_specs=(vmem, vmem),
        scratch_shapes=[
            pltpu.VMEM(couple_intersection.shape, bf16),
            pltpu.VMEM(pno_maps.shape, bf16),
            pltpu.VMEM((group_pairs, size, virtuals), bf16),
            pltpu.VMEM((group_pairs, size, size), bf16),
            pltpu.VMEM((group_pairs, size, size), bf16),
            pltpu.VMEM((SIDES * orbs, rows, virtuals), bf16),
            pltpu.VMEM((SIDES * orbs, rows, virtuals), bf16),
            pltpu.VMEM((group_pairs, rows, size), bf16),
            pltpu.VMEM((ITERS, ranks, own_pairs, size, size), bf16),
            pltpu.VMEM((ITERS, ranks, own_pairs, size, size), bf16),
            pltpu.VMEM((own_pairs, size, partners * size), bf16),
            pltpu.VMEM((orbs, rows, virtuals), jnp.float32),
            dma((ITERS, ranks, own_pairs)),
            dma((ITERS, ranks, own_pairs)),
            dma((ITERS, SIDES)),
            dma((ITERS, SIDES)),
            dma((ITERS, ranks)),
            dma((ITERS, ranks)),
            dma((own_pairs,)),
            dma((2,)),
            dma,
        ],
        compiler_params=pltpu.CompilerParams(
            collective_id=0, has_side_effects=True, vmem_limit_bytes=67043328
        ),
    )(
        couple,
        occ_first,
        occ_second,
        occ_energy,
        amplitudes,
        pno_energy,
        couple_intersection,
        pno_maps,
        orbital_blocks,
    )


def solution(mesh):
    return jax.shard_map(
        functools.partial(on_device, mesh.shape["orb"], mesh.shape["pair"]),
        mesh=mesh,
        in_specs=(
            P(("pair", "orb"), None, None),
            P(("pair", "orb"), None),
            P("pair"),
            P("pair"),
            P(("pair", "orb"), None, None, None),
            P("pair", None, None, None),
            P("pair", "orb", None),
            P(("pair", "orb"), None),
            P(),
        ),
        out_specs=(P(("pair", "orb"), None, None), P("pair", "orb", None)),
        check_vma=False,
    )
```

```python
import functools

import jax
import jax.numpy as jnp
from jax import lax
from jax.experimental import pallas as pl
from jax.experimental.pallas import tpu as pltpu
from jax.sharding import PartitionSpec as P

REACH = 1
ITERS = 2
SIDES = 2 * REACH + 1

dress_scale = 0.015

NN = (((1,), (0,)), ((), ()))
NT = (((1,), (1,)), ((), ()))


def dot(left, right, dims=NN):
    return lax.dot_general(left, right, dims, preferred_element_type=jnp.float32)


def kernel(
    ranks,
    groups,
    couple,
    occ_first,
    occ_second,
    occ_energy,
    amplitudes,
    pno_energy,
    inter_hbm,
    maps_hbm,
    orb_hbm,
    out_amps,
    out_dressed,
    inter,
    maps,
    first_t,
    amps_0,
    amps_1,
    window_0,
    window_1,
    second_z,
    parts_out,
    parts_in,
    half,
    fitted,
    amp_send,
    amp_recv,
    win_send,
    win_recv,
    part_send,
    part_recv,
    inter_sem,
    maps_sem,
    orb_sem,
):
    amps = (amps_0, amps_1)
    window = (window_0, window_1)
    own_pairs = amplitudes.shape[0]
    orbs = orb_hbm.shape[0]
    partners = couple.shape[1]
    size = amplitudes.shape[2]
    me = lax.axis_index("orb")
    group = lax.axis_index("pair")
    own = me * own_pairs
    own_rows = pl.ds(own, own_pairs)
    middle = pl.ds(REACH * orbs, orbs)
    bf16 = jnp.bfloat16
    square = ranks == 4 and own_pairs % 2 == 0
    low = own_pairs // 2
    lower, upper = pl.ds(0, low), pl.ds(low, own_pairs - low)

    def target(step):
        if square:
            return (me // 2 + step // 2) % 2 * 2 + (me + step) % 2
        return (me + step) % ranks

    def source(step):
        return target(step) if square else (me + ranks - step) % ranks

    orb_copy = pltpu.make_async_copy(orb_hbm, window[0].at[middle], orb_sem)
    orb_copy.start()
    maps_copies = []
    for part in range(2):
        chunk = pl.ds(part * (maps.shape[0] // 2), maps.shape[0] // 2)
        maps_copies.append(
            pltpu.make_async_copy(maps_hbm.at[chunk], maps.at[chunk], maps_sem.at[part])
        )
        maps_copies[-1].start()
    inter_copies = []
    for i in range(own_pairs):
        inter_copies.append(pltpu.make_async_copy(inter_hbm.at[i], inter.at[i], inter_sem.at[i]))
        inter_copies[-1].start()

    for i in range(own_pairs):
        amps[0][own + i] = amplitudes[i].astype(bf16)

    barrier = pltpu.get_barrier_semaphore()
    for step in range(1, ranks):
        pl.semaphore_signal(
            barrier,
            inc=1,
            device_id={"orb": (me + step) % ranks},
            device_id_type=pl.DeviceIdType.MESH,
        )
    for step in range(1, REACH + 1):
        for shift in (step, groups - step):
            pl.semaphore_signal(
                barrier,
                inc=1,
                device_id={"pair": (group + shift) % groups},
                device_id_type=pl.DeviceIdType.MESH,
            )
    pl.semaphore_wait(barrier, ranks - 1 + 2 * REACH)

    def win_copy(turn, place):
        return pltpu.make_async_remote_copy(
            src_ref=window[turn].at[middle],
            dst_ref=window[turn].at[pl.ds(place * orbs, orbs)],
            send_sem=win_send.at[turn, place],
            recv_sem=win_recv.at[turn, place],
            device_id={"pair": (group + REACH - place + groups) % groups},
            device_id_type=pl.DeviceIdType.MESH,
        )

    def amp_copy(turn, step, i):
        return pltpu.make_async_remote_copy(
            src_ref=amps[turn].at[own + i],
            dst_ref=amps[turn].at[own + i],
            send_sem=amp_send.at[turn, step, i],
            recv_sem=amp_recv.at[turn, step, i],
            device_id={"orb": target(step)},
            device_id_type=pl.DeviceIdType.MESH,
        )

    def amp_relay(turn, i):
        via, onto = (1, 2) if i < low else (2, 1)
        place = target(via) * own_pairs + i
        return pltpu.make_async_remote_copy(
            src_ref=amps[turn].at[place],
            dst_ref=amps[turn].at[place],
            send_sem=amp_send.at[turn, 3, i],
            recv_sem=amp_recv.at[turn, 3, i],
            device_id={"orb": target(onto)},
            device_id_type=pl.DeviceIdType.MESH,
        )

    def relay_all(turn):
        for i in range(low):
            for j, via in ((i, 1), (low + i, 2)):
                amp_copy(turn, via, j).wait_recv()
                amp_relay(turn, j).start()

    def amp_wait(turn, step):
        for i in range(own_pairs):
            if not square:
                amp_copy(turn, step, i).wait_recv()
            elif step == 3:
                amp_relay(turn, i).wait_recv()
            elif (i < low) != (step == 1):
                amp_copy(turn, step, i).wait_recv()

    def part_send_to(turn, step, onto, half_of, sem):
        rows = (slice(None), lower, upper)[half_of] if half_of else pl.ds(0, own_pairs)
        return pltpu.make_async_remote_copy(
            src_ref=parts_out.at[turn, step, rows],
            dst_ref=parts_in.at[turn, step, rows],
            send_sem=part_send.at[turn, sem],
            recv_sem=part_recv.at[turn, sem],
            device_id={"orb": target(onto)},
            device_id_type=pl.DeviceIdType.MESH,
        )

    if square:
        part_first = {1: [(1, 1, 1, 0)], 2: [(2, 2, 2, 1)], 3: [(3, 1, 1, 2), (3, 2, 2, 3)]}
        part_second = [(2, 2, 1, 4), (1, 1, 2, 5)]
        part_last = [(1, 1, 1, 0), (2, 2, 2, 1)] + part_second
        part_all = part_last + part_first[3]
        terms = (1, 2)
    else:
        part_first = {step: [(step, step, 0, step)] for step in range(1, ranks)}
        part_second = []
        part_last = part_all = [entry for step in part_first for entry in part_first[step]]
        terms = range(1, ranks)

    def part_forward(turn):
        for arrived, entry in zip((part_first[3] if square else []), part_second):
            part_send_to(turn, *arrived).wait_recv()
            step, _, half_of, _ = entry
            for i in range(low):
                i = i if half_of == 1 else low + i
                total = parts_out[turn, step, i].astype(jnp.float32)
                total += parts_in[turn, 3, i].astype(jnp.float32)
                parts_out[turn, step, i] = total.astype(bf16)
            part_send_to(turn, *entry).start()

    def amp_start(turn, i):
        for step in (1, 2) if square else range(1, ranks):
            amp_copy(turn, step, i).start()

    places = [place for place in range(SIDES) if place != REACH]

    orb_copy.wait()
    for place in places:
        win_copy(0, place).start()
    if square:
        for i in range(own_pairs):
            for step in (1, 2):
                j = i if step == 1 else (i + low) % own_pairs
                amp_copy(0, step, j).start()
    else:
        for i in range(own_pairs):
            amp_start(0, i)

    for copy in maps_copies:
        copy.wait()

    @pl.loop(0, ranks)
    def _(block):
        for i in range(own_pairs):
            first_t[block * own_pairs + i] = maps[block * own_pairs + i, 0].T

    for turn in range(ITERS):
        for place in places:
            win_copy(turn, place).wait_recv()
        if square and turn == 0:
            relay_all(turn)

        @pl.loop(1, ranks + 1)
        def _(ahead):
            step = ranks - ahead
            base = target(step) * own_pairs
            lefts, rights = [], []
            for i in range(own_pairs):
                pair = base + i
                first = REACH * orbs + occ_first[pair] % orbs
                second = occ_second[pair]
                distance = (second // orbs - group + REACH + groups) % groups
                place = jnp.minimum(distance, SIDES - 1)
                lefts.append(dot(first_t[pair], window[turn][first], NT).astype(bf16))
                rights.append(
                    dot(window[turn][place * orbs + second % orbs], maps[pair, 1]).astype(bf16)
                )
            for i in range(own_pairs):
                second_z[base + i] = rights[i]
                parts_out[turn, step, i] = dot(lefts[i], rights[i]).astype(bf16)

            if square:
                for at in part_first:

                    @pl.when(step == at)
                    def _(at=at):
                        for entry in part_first[at]:
                            part_send_to(turn, *entry).start()
            else:

                @pl.when(step > 0)
                def _():
                    part_send_to(turn, step, step, 0, step).start()

        if square and turn > 0:
            relay_all(turn)

        for o in range(orbs):
            fitted[o] = jnp.zeros_like(fitted[o])

        @pl.loop(0, ranks)
        def _(step):
            if square:
                for at in range(1, ranks):

                    @pl.when(step == at)
                    def _(at=at):
                        amp_wait(turn, at)
            else:

                @pl.when(step > 0)
                def _():
                    amp_wait(turn, step)

            base = source(step) * own_pairs
            halves = [
                dot(second_z[base + i], amps[turn][base + i]).astype(bf16)
                for i in range(own_pairs)
            ]
            returned = [dot(halves[i], first_t[base + i]) for i in range(own_pairs)]
            for o in range(orbs):
                total = fitted[o]
                for i in range(own_pairs):
                    weight = (occ_first[base + i] % orbs == o).astype(jnp.float32)
                    total += weight * returned[i]
                fitted[o] = total

        for o in range(orbs):
            value = window[0][REACH * orbs + o].astype(jnp.float32) + dress_scale * fitted[o]
            if turn + 1 < ITERS:
                window[turn + 1][REACH * orbs + o] = value.astype(bf16)
            else:
                out_dressed[o] = value
        if turn + 1 < ITERS:
            for place in places:
                win_copy(turn + 1, place).start()

        part_forward(turn)

        if turn == 0:
            for copy in inter_copies:
                copy.wait()

        @pl.loop(0, own_pairs)
        def _(i):
            for k in range(partners):
                partner = couple[i, k] % (ranks * own_pairs)
                half[i, :, k * size : (k + 1) * size] = dot(
                    inter[i, k], amps[turn][partner]
                ).astype(bf16)
            coupled = None
            for k in range(0, partners, 2):
                right = jnp.concatenate([inter[i, k], inter[i, k + 1]], axis=1)
                term = dot(half[i, :, k * size : (k + 2) * size], right, NT)
                coupled = term if coupled is None else coupled + term

            @pl.when(i == 0)
            def _():
                for entry in part_last:
                    part_send_to(turn, *entry).wait_recv()

            total = parts_out[turn, 0, i].astype(jnp.float32)
            for step in terms:
                total += parts_in[turn, step, i].astype(jnp.float32)
            rows = jnp.broadcast_to(pno_energy[pl.ds(i, 1), :], (size, size))
            denominator = rows + rows.T
            denominator -= occ_energy[occ_first[own + i]]
            denominator -= occ_energy[occ_second[own + i]]
            value = -(total + coupled) / denominator
            if turn + 1 < ITERS:
                amps[turn + 1][own + i] = value.astype(bf16)
                amp_start(turn + 1, i)
            else:
                out_amps[i] = value

    for turn in range(ITERS):
        for place in places:
            win_copy(turn, place).wait_send()
        for entry in part_all:
            part_send_to(turn, *entry).wait_send()
        for i in range(own_pairs):
            for step in range(1, ranks):
                if square and step == 3:
                    amp_relay(turn, i).wait_send()
                else:
                    amp_copy(turn, step, i).wait_send()


def on_device(
    ranks,
    groups,
    amplitudes,
    couple,
    occ_first,
    occ_second,
    couple_intersection,
    pno_maps,
    orbital_blocks,
    pno_energy,
    occ_energy,
):
    own_pairs, size, _ = amplitudes.shape
    group_pairs = occ_first.shape[0]
    orbs, rows, virtuals = orbital_blocks.shape
    partners = couple.shape[1]
    bf16 = jnp.bfloat16
    smem = pl.BlockSpec(memory_space=pltpu.SMEM)
    vmem = pl.BlockSpec(memory_space=pltpu.VMEM)
    hbm = pl.BlockSpec(memory_space=pltpu.HBM)
    dma = pltpu.SemaphoreType.DMA
    return pl.pallas_call(
        functools.partial(kernel, ranks, groups),
        out_shape=(
            jax.ShapeDtypeStruct(amplitudes.shape, jnp.float32),
            jax.ShapeDtypeStruct(orbital_blocks.shape, jnp.float32),
        ),
        in_specs=[smem] * 4 + [vmem] * 2 + [hbm] * 3,
        out_specs=(vmem, vmem),
        scratch_shapes=[
            pltpu.VMEM(couple_intersection.shape, bf16),
            pltpu.VMEM(pno_maps.shape, bf16),
            pltpu.VMEM((group_pairs, size, virtuals), bf16),
            pltpu.VMEM((group_pairs, size, size), bf16),
            pltpu.VMEM((group_pairs, size, size), bf16),
            pltpu.VMEM((SIDES * orbs, rows, virtuals), bf16),
            pltpu.VMEM((SIDES * orbs, rows, virtuals), bf16),
            pltpu.VMEM((group_pairs, rows, size), bf16),
            pltpu.VMEM((ITERS, ranks, own_pairs, size, size), bf16),
            pltpu.VMEM((ITERS, ranks, own_pairs, size, size), bf16),
            pltpu.VMEM((own_pairs, size, partners * size), bf16),
            pltpu.VMEM((orbs, rows, virtuals), jnp.float32),
            dma((ITERS, ranks, own_pairs)),
            dma((ITERS, ranks, own_pairs)),
            dma((ITERS, SIDES)),
            dma((ITERS, SIDES)),
            dma((ITERS, ranks + 2)),
            dma((ITERS, ranks + 2)),
            dma((own_pairs,)),
            dma((2,)),
            dma,
        ],
        compiler_params=pltpu.CompilerParams(
            collective_id=0, has_side_effects=True, vmem_limit_bytes=67043328
        ),
    )(
        couple,
        occ_first,
        occ_second,
        occ_energy,
        amplitudes,
        pno_energy,
        couple_intersection,
        pno_maps,
        orbital_blocks,
    )


def solution(mesh):
    return jax.shard_map(
        functools.partial(on_device, mesh.shape["orb"], mesh.shape["pair"]),
        mesh=mesh,
        in_specs=(
            P(("pair", "orb"), None, None),
            P(("pair", "orb"), None),
            P("pair"),
            P("pair"),
            P(("pair", "orb"), None, None, None),
            P("pair", None, None, None),
            P("pair", "orb", None),
            P(("pair", "orb"), None),
            P(),
        ),
        out_specs=(P(("pair", "orb"), None, None), P("pair", "orb", None)),
        check_vma=False,
    )
```

```python
import functools

import jax
import jax.numpy as jnp
from jax import lax
from jax.experimental import pallas as pl
from jax.experimental.pallas import tpu as pltpu
from jax.sharding import PartitionSpec as P

REACH = 1
ITERS = 2
SIDES = 2 * REACH + 1

dress_scale = 0.015

NN = (((1,), (0,)), ((), ()))
NT = (((1,), (1,)), ((), ()))


def dot(left, right, dims=NN):
    return lax.dot_general(left, right, dims, preferred_element_type=jnp.float32)


def kernel(
    ranks,
    groups,
    couple_hbm,
    first_hbm,
    second_hbm,
    energy_hbm,
    amps_hbm,
    pno_hbm,
    inter_hbm,
    maps_hbm,
    orb_hbm,
    out_amps,
    out_dressed,
    couple,
    occ_first,
    occ_second,
    occ_energy,
    amplitudes,
    pno_energy,
    inter,
    maps,
    first_t,
    amps_0,
    amps_1,
    window_0,
    window_1,
    second_z,
    parts_out,
    parts_in,
    half,
    fitted,
    amp_send,
    amp_recv,
    win_send,
    win_recv,
    part_send,
    part_recv,
    inter_sem,
    maps_sem,
    orb_sem,
    small_sem,
):
    amps = (amps_0, amps_1)
    window = (window_0, window_1)
    own_pairs = amps_hbm.shape[0]
    orbs = orb_hbm.shape[0]
    partners = couple.shape[1]
    size = amplitudes.shape[2]
    me = lax.axis_index("orb")
    group = lax.axis_index("pair")
    own = me * own_pairs
    own_rows = pl.ds(own, own_pairs)
    middle = pl.ds(REACH * orbs, orbs)
    bf16 = jnp.bfloat16
    square = ranks == 4 and own_pairs % 2 == 0
    low = own_pairs // 2
    lower, upper = pl.ds(0, low), pl.ds(low, own_pairs - low)

    def target(step):
        if square:
            return (me // 2 + step // 2) % 2 * 2 + (me + step) % 2
        return (me + step) % ranks

    def source(step):
        return target(step) if square else (me + ranks - step) % ranks

    orb_copy = pltpu.make_async_copy(orb_hbm, window[0].at[middle], orb_sem)
    orb_copy.start()
    small_copies = [
        pltpu.make_async_copy(source_ref, target_ref, small_sem.at[at])
        for at, (source_ref, target_ref) in enumerate(
            (
                (amps_hbm, amplitudes),
                (couple_hbm, couple),
                (first_hbm, occ_first),
                (second_hbm, occ_second),
                (energy_hbm, occ_energy),
                (pno_hbm, pno_energy),
            )
        )
    ]
    for copy in small_copies:
        copy.start()
    maps_copies = []
    for part in range(2):
        chunk = pl.ds(part * (maps.shape[0] // 2), maps.shape[0] // 2)
        maps_copies.append(
            pltpu.make_async_copy(maps_hbm.at[chunk], maps.at[chunk], maps_sem.at[part])
        )
        maps_copies[-1].start()
    inter_copies = []
    for i in range(own_pairs):
        inter_copies.append(pltpu.make_async_copy(inter_hbm.at[i], inter.at[i], inter_sem.at[i]))
        inter_copies[-1].start()

    barrier = pltpu.get_barrier_semaphore()
    for step in range(1, ranks):
        pl.semaphore_signal(
            barrier,
            inc=1,
            device_id={"orb": (me + step) % ranks},
            device_id_type=pl.DeviceIdType.MESH,
        )
    for step in range(1, REACH + 1):
        for shift in (step, groups - step):
            pl.semaphore_signal(
                barrier,
                inc=1,
                device_id={"pair": (group + shift) % groups},
                device_id_type=pl.DeviceIdType.MESH,
            )
    small_copies[0].wait()
    for i in range(own_pairs):
        amps[0][own + i] = amplitudes[i].astype(bf16)
    pl.semaphore_wait(barrier, ranks - 1 + 2 * REACH)

    def win_copy(turn, place):
        return pltpu.make_async_remote_copy(
            src_ref=window[turn].at[middle],
            dst_ref=window[turn].at[pl.ds(place * orbs, orbs)],
            send_sem=win_send.at[turn, place],
            recv_sem=win_recv.at[turn, place],
            device_id={"pair": (group + REACH - place + groups) % groups},
            device_id_type=pl.DeviceIdType.MESH,
        )

    def amp_copy(turn, step, i):
        return pltpu.make_async_remote_copy(
            src_ref=amps[turn].at[own + i],
            dst_ref=amps[turn].at[own + i],
            send_sem=amp_send.at[turn, step, i],
            recv_sem=amp_recv.at[turn, step, i],
            device_id={"orb": target(step)},
            device_id_type=pl.DeviceIdType.MESH,
        )

    def amp_relay(turn, i):
        via, onto = (1, 2) if i < low else (2, 1)
        place = target(via) * own_pairs + i
        return pltpu.make_async_remote_copy(
            src_ref=amps[turn].at[place],
            dst_ref=amps[turn].at[place],
            send_sem=amp_send.at[turn, 3, i],
            recv_sem=amp_recv.at[turn, 3, i],
            device_id={"orb": target(onto)},
            device_id_type=pl.DeviceIdType.MESH,
        )

    def relay_all(turn):
        for i in range(low):
            for j, via in ((i, 1), (low + i, 2)):
                amp_copy(turn, via, j).wait_recv()
                amp_relay(turn, j).start()

    def amp_wait(turn, step):
        for i in range(own_pairs):
            if not square:
                amp_copy(turn, step, i).wait_recv()
            elif step == 3:
                amp_relay(turn, i).wait_recv()
            elif (i < low) != (step == 1):
                amp_copy(turn, step, i).wait_recv()

    def part_send_to(turn, step, onto, half_of, sem):
        rows = (slice(None), lower, upper)[half_of] if half_of else pl.ds(0, own_pairs)
        return pltpu.make_async_remote_copy(
            src_ref=parts_out.at[turn, step, rows],
            dst_ref=parts_in.at[turn, step, rows],
            send_sem=part_send.at[turn, sem],
            recv_sem=part_recv.at[turn, sem],
            device_id={"orb": target(onto)},
            device_id_type=pl.DeviceIdType.MESH,
        )

    if square:
        part_first = {1: [(1, 1, 1, 0)], 2: [(2, 2, 2, 1)], 3: [(3, 1, 1, 2), (3, 2, 2, 3)]}
        part_second = [(2, 2, 1, 4), (1, 1, 2, 5)]
        part_last = [(1, 1, 1, 0), (2, 2, 2, 1)] + part_second
        part_all = part_last + part_first[3]
        terms = (1, 2)
    else:
        part_first = {step: [(step, step, 0, step)] for step in range(1, ranks)}
        part_second = []
        part_last = part_all = [entry for step in part_first for entry in part_first[step]]
        terms = range(1, ranks)

    def part_forward(turn):
        for arrived, entry in zip((part_first[3] if square else []), part_second):
            part_send_to(turn, *arrived).wait_recv()
            step, _, half_of, _ = entry
            for i in range(low):
                i = i if half_of == 1 else low + i
                total = parts_out[turn, step, i].astype(jnp.float32)
                total += parts_in[turn, 3, i].astype(jnp.float32)
                parts_out[turn, step, i] = total.astype(bf16)
            part_send_to(turn, *entry).start()

    def amp_start(turn, i):
        for step in (1, 2) if square else range(1, ranks):
            amp_copy(turn, step, i).start()

    places = [place for place in range(SIDES) if place != REACH]

    orb_copy.wait()
    for place in places:
        win_copy(0, place).start()
    if square:
        for i in range(own_pairs):
            for step in (1, 2):
                j = i if step == 1 else (i + low) % own_pairs
                amp_copy(0, step, j).start()
    else:
        for i in range(own_pairs):
            amp_start(0, i)

    for copy in maps_copies + small_copies[1:]:
        copy.wait()

    @pl.loop(0, ranks)
    def _(block):
        for i in range(own_pairs):
            first_t[block * own_pairs + i] = maps[block * own_pairs + i, 0].T

    for turn in range(ITERS):
        for place in places:
            win_copy(turn, place).wait_recv()
        if square and turn == 0:
            relay_all(turn)

        @pl.loop(1, ranks + 1)
        def _(ahead):
            step = ranks - ahead
            base = target(step) * own_pairs
            lefts, rights = [], []
            for i in range(own_pairs):
                pair = base + i
                first = REACH * orbs + occ_first[pair] % orbs
                second = occ_second[pair]
                distance = (second // orbs - group + REACH + groups) % groups
                place = jnp.minimum(distance, SIDES - 1)
                lefts.append(dot(first_t[pair], window[turn][first], NT).astype(bf16))
                rights.append(
                    dot(window[turn][place * orbs + second % orbs], maps[pair, 1]).astype(bf16)
                )
            for i in range(own_pairs):
                second_z[base + i] = rights[i]
                parts_out[turn, step, i] = dot(lefts[i], rights[i]).astype(bf16)

            if square:
                for at in part_first:

                    @pl.when(step == at)
                    def _(at=at):
                        for entry in part_first[at]:
                            part_send_to(turn, *entry).start()
            else:

                @pl.when(step > 0)
                def _():
                    part_send_to(turn, step, step, 0, step).start()

        if square and turn > 0:
            relay_all(turn)

        for o in range(orbs):
            fitted[o] = jnp.zeros_like(fitted[o])

        @pl.loop(0, ranks)
        def _(step):
            if square:
                for at in range(1, ranks):

                    @pl.when(step == at)
                    def _(at=at):
                        amp_wait(turn, at)
            else:

                @pl.when(step > 0)
                def _():
                    amp_wait(turn, step)

            base = source(step) * own_pairs
            halves = [
                dot(second_z[base + i], amps[turn][base + i]).astype(bf16)
                for i in range(own_pairs)
            ]
            returned = [dot(halves[i], first_t[base + i]) for i in range(own_pairs)]
            for o in range(orbs):
                total = fitted[o]
                for i in range(own_pairs):
                    weight = (occ_first[base + i] % orbs == o).astype(jnp.float32)
                    total += weight * returned[i]
                fitted[o] = total

        for o in range(orbs):
            value = window[0][REACH * orbs + o].astype(jnp.float32) + dress_scale * fitted[o]
            if turn + 1 < ITERS:
                window[turn + 1][REACH * orbs + o] = value.astype(bf16)
            else:
                out_dressed[o] = value
        if turn + 1 < ITERS:
            for place in places:
                win_copy(turn + 1, place).start()

        part_forward(turn)

        if turn == 0:
            for copy in inter_copies:
                copy.wait()

        @pl.loop(0, own_pairs)
        def _(i):
            for k in range(partners):
                partner = couple[i, k] % (ranks * own_pairs)
                half[i, :, k * size : (k + 1) * size] = dot(
                    inter[i, k], amps[turn][partner]
                ).astype(bf16)
            coupled = None
            for k in range(0, partners, 2):
                right = jnp.concatenate([inter[i, k], inter[i, k + 1]], axis=1)
                term = dot(half[i, :, k * size : (k + 2) * size], right, NT)
                coupled = term if coupled is None else coupled + term

            @pl.when(i == 0)
            def _():
                for entry in part_last:
                    part_send_to(turn, *entry).wait_recv()

            total = parts_out[turn, 0, i].astype(jnp.float32)
            for step in terms:
                total += parts_in[turn, step, i].astype(jnp.float32)
            rows = jnp.broadcast_to(pno_energy[pl.ds(i, 1), :], (size, size))
            denominator = rows + rows.T
            denominator -= occ_energy[occ_first[own + i]]
            denominator -= occ_energy[occ_second[own + i]]
            value = -(total + coupled) / denominator
            if turn + 1 < ITERS:
                amps[turn + 1][own + i] = value.astype(bf16)
                amp_start(turn + 1, i)
            else:
                out_amps[i] = value

    for turn in range(ITERS):
        for place in places:
            win_copy(turn, place).wait_send()
        for entry in part_all:
            part_send_to(turn, *entry).wait_send()
        for i in range(own_pairs):
            for step in range(1, ranks):
                if square and step == 3:
                    amp_relay(turn, i).wait_send()
                else:
                    amp_copy(turn, step, i).wait_send()


def on_device(
    ranks,
    groups,
    amplitudes,
    couple,
    occ_first,
    occ_second,
    couple_intersection,
    pno_maps,
    orbital_blocks,
    pno_energy,
    occ_energy,
):
    own_pairs, size, _ = amplitudes.shape
    group_pairs = occ_first.shape[0]
    orbs, rows, virtuals = orbital_blocks.shape
    partners = couple.shape[1]
    bf16 = jnp.bfloat16
    vmem = pl.BlockSpec(memory_space=pltpu.VMEM)
    hbm = pl.BlockSpec(memory_space=pltpu.HBM)
    dma = pltpu.SemaphoreType.DMA
    return pl.pallas_call(
        functools.partial(kernel, ranks, groups),
        out_shape=(
            pltpu.VMEM(amplitudes.shape, jnp.float32),
            pltpu.VMEM(orbital_blocks.shape, jnp.float32),
        ),
        in_specs=[hbm] * 9,
        out_specs=(vmem, vmem),
        scratch_shapes=[
            pltpu.SMEM(couple.shape, couple.dtype),
            pltpu.SMEM(occ_first.shape, occ_first.dtype),
            pltpu.SMEM(occ_second.shape, occ_second.dtype),
            pltpu.SMEM(occ_energy.shape, occ_energy.dtype),
            pltpu.VMEM(amplitudes.shape, amplitudes.dtype),
            pltpu.VMEM(pno_energy.shape, pno_energy.dtype),
            pltpu.VMEM(couple_intersection.shape, bf16),
            pltpu.VMEM(pno_maps.shape, bf16),
            pltpu.VMEM((group_pairs, size, virtuals), bf16),
            pltpu.VMEM((group_pairs, size, size), bf16),
            pltpu.VMEM((group_pairs, size, size), bf16),
            pltpu.VMEM((SIDES * orbs, rows, virtuals), bf16),
            pltpu.VMEM((SIDES * orbs, rows, virtuals), bf16),
            pltpu.VMEM((group_pairs, rows, size), bf16),
            pltpu.VMEM((ITERS, ranks, own_pairs, size, size), bf16),
            pltpu.VMEM((ITERS, ranks, own_pairs, size, size), bf16),
            pltpu.VMEM((own_pairs, size, partners * size), bf16),
            pltpu.VMEM((orbs, rows, virtuals), jnp.float32),
            dma((ITERS, ranks, own_pairs)),
            dma((ITERS, ranks, own_pairs)),
            dma((ITERS, SIDES)),
            dma((ITERS, SIDES)),
            dma((ITERS, ranks + 2)),
            dma((ITERS, ranks + 2)),
            dma((own_pairs,)),
            dma((2,)),
            dma,
            dma((6,)),
        ],
        compiler_params=pltpu.CompilerParams(
            collective_id=0, has_side_effects=True, vmem_limit_bytes=67043328 - 4096 * 1024
        ),
    )(
        *(pltpu.with_memory_space_constraint(x, pltpu.HBM) for x in (
        couple,
        occ_first,
        occ_second,
        occ_energy,
        amplitudes,
        pno_energy,
        couple_intersection,
        pno_maps,
        orbital_blocks,
        ))
    )


def solution(mesh):
    return jax.shard_map(
        functools.partial(on_device, mesh.shape["orb"], mesh.shape["pair"]),
        mesh=mesh,
        in_specs=(
            P(("pair", "orb"), None, None),
            P(("pair", "orb"), None),
            P("pair"),
            P("pair"),
            P(("pair", "orb"), None, None, None),
            P("pair", None, None, None),
            P("pair", "orb", None),
            P(("pair", "orb"), None),
            P(),
        ),
        out_specs=(P(("pair", "orb"), None, None), P("pair", "orb", None)),
        check_vma=False,
    )
```
